32 devices in a mesh: dp: 2 (over x), expert: 16 (over z, y, core).
Axes of the slice: x: 2, y: 2, z: 4, core: 2. Of those that a mesh axis runs over, the one named last changes fastest.
Arguments:
- tokens: bfloat16 [3072, 2048], P(('dp', 'expert')), may hold values from -6 to 6
- routes: int32 [3072, 8], P(('dp', 'expert')), may hold values from 0 to 15, all different within a row; in each aligned block of 96 rows (0 to 95, 96 to 191, ...) at most 64 rows name the same one
- weights: bfloat16 [16, 2, 768, 2048], P('expert', None, 'dp'), may hold values from -0.125 to 0.125
- keep_mask: int32 [16, 2, 768, 128], P('expert', None, 'dp'), may hold values from 0 to 1, as said below
- inv_factor: float32 [16, 128, 2048], P('expert'), as said below
Outputs:
- hidden: bfloat16 [3072, 8, 768], P(('dp', 'expert'))
The draws below stay inside these ranges and needn't reach their ends.
Inputs may be any that keep to these rules, and one draw needn't show every extreme that they name: `routes`: each token names 8 different experts; the 96 rows of one device name any one expert at most 64 times. `keep_mask`: each row of 128 entries holds exactly 64 ones. `inv_factor`: each expert's factor is upper triangular: entry (i, j) is zero for j < i, and the diagonal entry (i, i) lies in [0.6, 1.6].
All inputs are finite; a program needn't handle non-finite values.
Results may differ from the reference program's by a relative error of at most 0.0058.
Values may be sent and summed in bfloat16 or wider, within the bound.
A program may use at most 64 MiB of HBM per device.

```python
import math
import jax
import jax.numpy as jnp
import numpy as np
from jax import lax

D = 2048
FW = 768
TOP = 8
BLOCK = 128
KEEP = 64
TOK_DEV = 96
EXPERTS = 16
CAP = 64
TOKENS = 3072
N_DP = 2
N_EXPERT = 16


def draw_keep_mask(key, part):
    key_list = jax.random.split(jax.random.fold_in(key, 11), EXPERTS * 2 * FW)
    orders = jax.vmap(lambda single: jax.random.permutation(single, BLOCK))(key_list)
    return (orders < KEEP).astype(jnp.int32).reshape(EXPERTS, 2, FW, BLOCK)


def draw_inv_factor(key, part):
    first, second, third = jax.random.split(jax.random.fold_in(key, 23), 3)
    diag_vec = jnp.exp(jax.random.uniform(first, (EXPERTS, BLOCK), jnp.float32, jnp.log(0.6), jnp.log(1.6)))
    spread = 0.1 * jax.random.normal(second, (EXPERTS, BLOCK, D), jnp.float32)
    rates = jax.random.uniform(third, (EXPERTS, BLOCK), jnp.float32, 0.15, 0.35)
    col_diag = jnp.concatenate([diag_vec, jnp.zeros((EXPERTS, D - BLOCK), jnp.float32)], axis=1)
    leak = rates[:, :, None] * col_diag[:, None, :]
    row_ids = jnp.arange(BLOCK)[None, :, None]
    col_ids = jnp.arange(D)[None, None, :]
    factor = jnp.where(col_ids == row_ids, diag_vec[:, :, None], jnp.where(col_ids > row_ids, leak + spread, 0.0))
    return factor.astype(jnp.float32)


def levels(key, shape, cuts, least, high):
    loudness = 1.0
    for dim, parts in cuts:
        heights = jax.random.uniform(jax.random.fold_in(jax.random.fold_in(key, 6), dim), (parts,), jnp.float32, least / len(cuts), high / len(cuts))
        loudness = loudness * jnp.repeat(jnp.exp(heights), shape[dim] // parts).reshape((-1,) + (1,) * (len(shape) - 1 - dim))
    return loudness


def deal_out(key, own, number, rows, amount, top, bound, lean):
    sequence = jax.random.permutation(key, amount)
    crowded, usual = shares(amount, rows * top, bound, lean, True), shares(amount, rows * top, bound, lean, False)
    places = jnp.arange(amount)

    def named(tallies, rotation):
        used = int((tallies > 0).sum())
        fixed = max(1, used // 4)
        shifted = fixed + (places - fixed + rotation * (used - fixed)) % max(1, amount - fixed)
        return jnp.zeros((amount,), jnp.int32).at[sequence[jnp.where(places < fixed, places, shifted)]].set(jnp.asarray(tallies, jnp.int32))

    tallies = jnp.where(number % 4 == 0, named(crowded, number // 4), named(usual, number - number // 4 - 1))
    mixed = jax.random.permutation(jax.random.fold_in(own, 3), amount)
    giver, sink = mixed[0:amount // 2 * 2:2], mixed[1:amount // 2 * 2:2]
    margin = jnp.minimum(tallies[giver] - 1, bound - tallies[sink]) // 2
    margin = jnp.where((giver == sequence[0]) | (sink == sequence[0]) | (tallies[sink] == 0), 0, jnp.maximum(margin, 0))
    shifted = jax.random.randint(jax.random.fold_in(own, 4), (amount // 2,), 0, 1 << 20) % (margin + 1)
    tallies = tallies.at[giver].add(-shifted).at[sink].add(shifted)
    items = jnp.searchsorted(jnp.cumsum(tallies), jnp.arange(rows * top), side="right").astype(jnp.int32)
    listing = items.reshape(top, rows).T
    listing = listing[jax.random.permutation(jax.random.fold_in(own, 1), rows)]
    rotation = jax.random.randint(jax.random.fold_in(own, 2), (rows, 1), 0, top)
    return jnp.take_along_axis(listing, (jnp.arange(top)[None, :] + rotation) % top, axis=1)


def shares(number_of, total, reach, skew, full):
    portions = [(1 << 20) // math.isqrt(standing ** skew) + 1 for standing in range(1, number_of + 1)]
    largest = reach if full else min(reach, max(-(-total // number_of), total * portions[0] // sum(portions)))
    least = 1 if total - largest >= number_of - 1 else 0
    holding, surplus = [largest] + [least] * (number_of - 1), total - largest - least * (number_of - 1)
    while surplus > 0:
        candidates = [i for i in range(1, number_of) if holding[i] < largest] or [i for i in range(1, number_of) if holding[i] < reach]
        whole, budget = sum([portions[i] for i in candidates]), surplus
        for i in candidates:
            addition = min(reach - holding[i], max(1, budget * portions[i] // whole), surplus)
            holding[i] = holding[i] + addition
            surplus = surplus - addition
    return np.array(holding)


def scatter_about(key, dims, deviation, limit, cuts=(), kind=jnp.bfloat16):
    drawn = deviation * jax.random.normal(key, dims, jnp.float32)
    if cuts:
        drawn = drawn * levels(key, dims, cuts, -0.22, 0.18)
    return jnp.clip(drawn, -limit, limit).astype(kind)


def setup_inputs(seed: int = 0) -> dict:
    streams_of = jax.random.split(jax.random.key(seed), 6)
    tokens = scatter_about(streams_of[0], (TOKENS, D), 1.0, 6.0, ((0, 32),))
    routes_keys = jax.random.split(jax.random.fold_in(streams_of[1], 1), TOKENS // TOK_DEV)
    routes_turns = jax.random.permutation(jax.random.fold_in(streams_of[1], 3), TOKENS // TOK_DEV)
    routes = jax.vmap(lambda own, number: deal_out(jax.random.fold_in(streams_of[1], 2), own, number, TOK_DEV, EXPERTS, TOP, CAP, 1))(routes_keys, routes_turns).reshape((TOKENS, TOP))
    weights = scatter_about(streams_of[2], (EXPERTS, 2, FW, D), D ** -0.5, 0.125, ((0, 16), (2, 2)))
    keep_mask = draw_keep_mask(jax.random.fold_in(streams_of[5], 71), 0)
    inv_factor = draw_inv_factor(jax.random.fold_in(streams_of[5], 71), 0)
    return dict(tokens=tokens, routes=routes, weights=weights, keep_mask=keep_mask, inv_factor=inv_factor)


def prune_rows(weights, keep_mask, inv_factor):
    block_width = keep_mask.shape[-1]
    initial = weights.astype(jnp.float32)
    leading = initial[..., :block_width]
    dropped = (1 - keep_mask).astype(jnp.float32)
    factor_block = inv_factor[:, :, :block_width]

    def column(column_id, state):
        leading, errors = state
        current = lax.dynamic_index_in_dim(leading, column_id, 3, keepdims=False)
        factor_row = lax.dynamic_index_in_dim(factor_block, column_id, 1, keepdims=False)
        diagonal = lax.dynamic_index_in_dim(factor_row, column_id, 1, keepdims=False)
        error_col = lax.dynamic_index_in_dim(dropped, column_id, 3, keepdims=False) * current / diagonal[:, None, None]
        leading = leading - error_col[..., None] * factor_row[:, None, None, :]
        errors = lax.dynamic_update_index_in_dim(errors, error_col, column_id, 3)
        return leading, errors

    leading, errors = lax.fori_loop(0, block_width, column, (leading, jnp.zeros_like(leading)))
    trailing = initial[..., block_width:] - jnp.einsum("epri,eij->eprj", errors, inv_factor[:, :, block_width:], precision=lax.Precision.HIGHEST)
    return jnp.concatenate([leading, trailing], axis=-1).astype(jnp.bfloat16)


def reference(tokens, routes, weights, keep_mask, inv_factor):
    def prune_one(packed):
        return prune_rows(packed[0][None], packed[1][None], packed[2][None])[0]

    pruned = lax.map(prune_one, (weights, keep_mask, inv_factor))
    slot_expert = routes.reshape(-1).astype(jnp.int32)
    slot_total = slot_expert.shape[0]
    by_expert = jnp.argsort(slot_expert, stable=True).astype(jnp.int32)
    per_expert = jnp.bincount(slot_expert, length=EXPERTS).astype(jnp.int32)
    expert_start = (jnp.cumsum(per_expert) - per_expert).astype(jnp.int32)
    group_rows = CAP * N_DP * N_EXPERT
    padded_order = jnp.concatenate([by_expert, jnp.full((group_rows,), slot_total, jnp.int32)])

    def expert_step(hidden_all, expert_id):
        slot_ids = lax.dynamic_slice_in_dim(padded_order, expert_start[expert_id], group_rows)
        is_live = jnp.arange(group_rows, dtype=jnp.int32) < per_expert[expert_id]
        slot_ids = jnp.where(is_live, slot_ids, slot_total).astype(jnp.int32)
        chosen = tokens[jnp.minimum(slot_ids, slot_total - 1) // TOP].astype(jnp.float32)
        gate_out = jnp.dot(chosen, pruned[expert_id, 0].astype(jnp.float32).T, preferred_element_type=jnp.float32)
        up_out = jnp.dot(chosen, pruned[expert_id, 1].astype(jnp.float32).T, preferred_element_type=jnp.float32)
        hidden_rows = (jax.nn.silu(gate_out) * up_out).astype(jnp.bfloat16)
        hidden_all = hidden_all.at[slot_ids].set(hidden_rows, mode="drop")
        return hidden_all, None

    hidden_all = jnp.zeros((slot_total, FW), jnp.bfloat16)
    hidden_all, _ = lax.scan(expert_step, hidden_all, jnp.arange(EXPERTS, dtype=jnp.int32))
    return hidden_all.reshape(TOKENS, TOP, FW)
```

```python
import functools

import jax
import jax.numpy as jnp
from jax import lax
from jax.experimental import pallas as pl
from jax.experimental.pallas import tpu as pltpu
from jax.sharding import PartitionSpec as P

SUB = 8
LANES = 128
GATHER_LIMIT = 24 << 20
VMEM = pltpu.VMEM


def prune_kernel(w_ref, mask_ref, f_ref, out_ref, u_ref, e_ref, m_ref, ft_ref, lhs_ref, rhs_ref):
    rows, width = w_ref.shape
    block = mask_ref.shape[1]
    blocks = block // SUB
    u_ref[...] = w_ref[:, :block].astype(jnp.float32).T
    factor = f_ref[:, :block]
    eye = lax.broadcasted_iota(jnp.int32, (block, block), 0) == lax.broadcasted_iota(
        jnp.int32, (block, block), 1
    )
    diagonal = jnp.sum(jnp.where(eye, factor, 0.0), axis=1, keepdims=True)
    m_ref[...] = (1 - mask_ref[...]).astype(jnp.float32).T * (1.0 / diagonal)
    factor_t = factor.T
    for b in range(blocks):
        ft_ref[b, :, :SUB] = factor_t[:, b * SUB : (b + 1) * SUB]

    def outer(b, carry):
        start = pl.multiple_of(b * SUB, SUB)
        u = u_ref[pl.ds(start, SUB), :]
        m = m_ref[pl.ds(start, SUB), :]
        ft = ft_ref[b, pl.ds(start, SUB), :SUB]
        errors = []
        for s in range(SUB):
            error = jnp.broadcast_to(m[s : s + 1] * u[s : s + 1], (SUB, rows))
            u = u - ft[:, s : s + 1] * error
            errors.append(error)
        u_ref[pl.ds(start, SUB), :] = u
        sub_ids = lax.broadcasted_iota(jnp.int32, (SUB, rows), 0)
        stacked = errors[0]
        for s in range(1, SUB):
            stacked = jnp.where(sub_ids == s, errors[s], stacked)
        e_ref[pl.ds(start, SUB), :] = stacked

        def inner(c, carry):
            place = pl.multiple_of(c * SUB, SUB)
            later = u_ref[pl.ds(place, SUB), :]
            column = ft_ref[b, pl.ds(place, SUB), :SUB]
            for s in range(SUB):
                later = later - column[:, s : s + 1] * errors[s]
            u_ref[pl.ds(place, SUB), :] = later
            return carry

        return lax.fori_loop(b + 1, blocks, inner, carry)

    lax.fori_loop(0, blocks, outer, 0)
    errors = e_ref[...].T
    high = errors.astype(jnp.bfloat16)
    low = (errors - high.astype(jnp.float32)).astype(jnp.bfloat16)
    lhs_ref[:, :block] = high
    lhs_ref[:, block : 2 * block] = low
    lhs_ref[:, 2 * block :] = high
    f_high = f_ref[...].astype(jnp.bfloat16)
    f_low = (f_ref[...] - f_high.astype(jnp.float32)).astype(jnp.bfloat16)
    rhs_ref[:block] = f_high
    rhs_ref[block : 2 * block] = f_high
    rhs_ref[2 * block :] = f_low
    out_ref[:, :block] = u_ref[...].T.astype(jnp.bfloat16)
    tile = next(t for t in (3 * LANES, 2 * LANES, LANES) if (width - block) % t == 0)

    def trail(c, carry):
        cols = pl.ds(pl.multiple_of(block + c * tile, LANES), tile)
        change = jnp.dot(lhs_ref[...], rhs_ref[:, cols], preferred_element_type=jnp.float32)
        out_ref[:, cols] = (w_ref[:, cols].astype(jnp.float32) - change).astype(jnp.bfloat16)
        return carry

    lax.fori_loop(0, (width - block) // tile, trail, 0)


def prune(weights, keep_mask, inv_factor):
    rows, width = weights.shape
    block = keep_mask.shape[1]
    return pl.pallas_call(
        prune_kernel,
        out_shape=jax.ShapeDtypeStruct((rows, width), jnp.bfloat16),
        in_specs=[pl.BlockSpec(memory_space=VMEM)] * 3,
        out_specs=pl.BlockSpec(memory_space=VMEM),
        scratch_shapes=[
            VMEM((block, rows), jnp.float32),
            VMEM((block, rows), jnp.float32),
            VMEM((block, rows), jnp.float32),
            VMEM((block // SUB, block, LANES), jnp.float32),
            VMEM((rows, 3 * block), jnp.bfloat16),
            VMEM((3 * block, width), jnp.bfloat16),
        ],
        cost_estimate=pl.CostEstimate(
            flops=6 * rows * block * width, bytes_accessed=4 * rows * width, transcendentals=0
        ),
        name="prune",
    )(weights, keep_mask, inv_factor)


def apply_kernel(capacity, token_rows, x_ref, w_ref, out_ref):
    width = w_ref.shape[1]
    half = w_ref.shape[0] // 2
    expert = lax.axis_index("expert")
    x = x_ref[:, :width]
    both = lax.dot_general(
        x, w_ref[...], (((1,), (1,)), ((), ())), preferred_element_type=jnp.float32
    )
    gate, up = both[:, :half], both[:, half:]
    hidden = (gate / (1.0 + jnp.exp(-gate)) * up).astype(jnp.bfloat16)
    ranks = x_ref[:, width:].astype(jnp.float32)
    lane = lax.broadcasted_iota(jnp.int32, ranks.shape, 1)
    rank = jnp.sum(jnp.where(lane == expert, ranks, 0.0), axis=1, keepdims=True).astype(jnp.int32)
    slots = lax.broadcasted_iota(jnp.int32, (x.shape[0], capacity), 1)
    pick = jnp.where(rank == slots, 1.0, 0.0).astype(jnp.bfloat16)
    for j in range(x.shape[0] // token_rows):
        part = slice(j * token_rows, (j + 1) * token_rows)
        out_ref[j] = lax.dot_general(
            pick[part], hidden[part], (((0,), (0,)), ((), ())), preferred_element_type=jnp.float32
        ).astype(jnp.bfloat16)


def combine_kernel(target_ref, got_ref, out_ref):
    halves, slots, half = got_ref.shape
    place = lax.broadcasted_iota(jnp.int32, (target_ref.shape[0], slots), 1)
    pick = jnp.where(target_ref[...] == place, 1.0, 0.0).astype(jnp.bfloat16)
    for h in range(halves):
        out_ref[:, h * half : (h + 1) * half] = jnp.dot(
            pick, got_ref[h], preferred_element_type=jnp.float32
        ).astype(jnp.bfloat16)


def ranks_of(routes, owners):
    token_rows = routes.shape[0]
    ids = jnp.arange(owners, dtype=jnp.int32)
    hot = jnp.any(routes[:, :, None] == ids[None, None, :], axis=1)
    before = jnp.tril(jnp.ones((token_rows, token_rows), jnp.bfloat16), -1)
    rank = jnp.dot(before, hot.astype(jnp.bfloat16), preferred_element_type=jnp.float32)
    return jnp.where(hot, rank, -1.0)


def dense(tokens, routes, pruned, capacity):
    owners, groups = lax.axis_size("expert"), lax.axis_size("dp")
    token_rows, width = tokens.shape
    top = routes.shape[1]
    devices = owners * groups
    half = pruned.shape[0] // 2
    rank = ranks_of(routes, owners)
    extra = -owners % LANES
    tagged = jnp.concatenate(
        [tokens, jnp.pad(rank, ((0, 0), (0, extra))).astype(jnp.bfloat16)], axis=1
    )
    gathered = lax.all_gather(tagged, ("dp", "expert"), axis=0, tiled=True)
    many = next(m for m in (4, 2, 1) if devices % m == 0)
    packed = pl.pallas_call(
        functools.partial(apply_kernel, capacity, token_rows),
        grid=(devices // many,),
        out_shape=jax.ShapeDtypeStruct((devices, capacity, half), jnp.bfloat16),
        in_specs=[
            pl.BlockSpec((many * token_rows, tagged.shape[1]), lambda i: (i, 0)),
            pl.BlockSpec((2 * half, width), lambda i: (0, 0)),
        ],
        out_specs=pl.BlockSpec((many, capacity, half), lambda i: (i, 0, 0)),
        name="apply",
    )(gathered, pruned)
    got = lax.all_to_all(packed, ("dp", "expert"), split_axis=0, concat_axis=0, tiled=True)
    ids = jnp.arange(owners, dtype=jnp.int32)
    own_rank = jnp.sum(
        jnp.where(routes[:, :, None] == ids[None, None, :], rank[:, None, :], 0.0), axis=2
    ).astype(jnp.int32)
    target = (routes * capacity + own_rank).reshape(-1, 1)
    out = pl.pallas_call(
        combine_kernel,
        out_shape=jax.ShapeDtypeStruct((token_rows * top, groups * half), jnp.bfloat16),
        name="combine",
    )(target, got.reshape(groups, owners * capacity, half))
    return out.reshape(token_rows, top, groups * half)


def routed(tokens, routes, pruned, capacity):
    half = pruned.shape[0] // 2
    gate_all = lax.all_gather(pruned[:half], "dp", axis=0, tiled=True)
    up_all = lax.all_gather(pruned[half:], "dp", axis=0, tiled=True)
    owners = lax.axis_size("expert")
    token_rows, model_width = tokens.shape
    top_count = routes.shape[1]
    slot_expert = routes.reshape(-1)
    one_hot = (slot_expert[:, None] == jnp.arange(owners, dtype=jnp.int32)[None, :]).astype(
        jnp.int32
    )
    slot_rank = jnp.sum(jnp.cumsum(one_hot, axis=0) * one_hot, axis=1) - 1
    target = slot_expert * capacity + slot_rank
    source = jnp.arange(slot_expert.shape[0], dtype=jnp.int32) // top_count
    outbox = (
        jnp.zeros((owners * capacity, model_width), jnp.bfloat16).at[target].set(tokens[source])
    )
    outbox = outbox.reshape(owners, capacity, model_width)
    arrived = lax.all_to_all(outbox, "expert", split_axis=0, concat_axis=0, tiled=True)
    arrived_rows = arrived.reshape(-1, model_width)
    gate_out = lax.dot_general(
        arrived_rows, gate_all, (((1,), (1,)), ((), ())), preferred_element_type=jnp.float32
    )
    up_out = lax.dot_general(
        arrived_rows, up_all, (((1,), (1,)), ((), ())), preferred_element_type=jnp.float32
    )
    hidden_rows = (jax.nn.silu(gate_out) * up_out).astype(jnp.bfloat16)
    hidden_rows = hidden_rows.reshape(arrived.shape[0], arrived.shape[1], -1)
    results = lax.all_to_all(hidden_rows, "expert", split_axis=0, concat_axis=0, tiled=True)
    hidden = results.reshape(owners * capacity, -1)[target]
    return hidden.reshape(token_rows, top_count, -1)


def local(tokens, routes, weights, keep_mask, inv_factor):
    owners, groups = lax.axis_size("expert"), lax.axis_size("dp")
    token_rows, width = tokens.shape
    capacity = token_rows * routes.shape[1] * 4 // (3 * owners)
    pruned = prune(
        weights.reshape(-1, width),
        keep_mask.reshape(-1, keep_mask.shape[-1]),
        inv_factor.reshape(-1, width),
    )
    if 2 * owners * groups * tokens.size <= GATHER_LIMIT:
        return dense(tokens, routes, pruned, capacity)
    return routed(tokens, routes, pruned, capacity)


def solution(mesh):
    return jax.shard_map(
        local,
        mesh=mesh,
        in_specs=(
            P(("dp", "expert"), None),
            P(("dp", "expert"), None),
            P("expert", None, "dp", None),
            P("expert", None, "dp", None),
            P("expert", None, None),
        ),
        out_specs=P(("dp", "expert"), None, None),
        check_vma=False,
    )
```

```python
import functools

import jax
import jax.numpy as jnp
from jax import lax
from jax.experimental import pallas as pl
from jax.experimental.pallas import tpu as pltpu
from jax.sharding import PartitionSpec as P

SUB = 8
LANES = 128
GATHER_LIMIT = 24 << 20
VMEM = pltpu.VMEM


def prune_setup(w_ref, mask_ref, f_ref, u_ref, m_ref, ft_ref):
    block = mask_ref.shape[1]
    u_ref[...] = w_ref[:, :block].astype(jnp.float32).T
    factor = f_ref[:, :block]
    eye = lax.broadcasted_iota(jnp.int32, (block, block), 0) == lax.broadcasted_iota(
        jnp.int32, (block, block), 1
    )
    diagonal = jnp.sum(jnp.where(eye, factor, 0.0), axis=1, keepdims=True)
    m_ref[...] = (1 - mask_ref[...]).astype(jnp.float32).T * (1.0 / diagonal)
    factor_t = factor.T
    for b in range(block // SUB):
        ft_ref[b, :, :SUB] = factor_t[:, b * SUB : (b + 1) * SUB]


def prune_columns(first, last, u_ref, e_ref, m_ref, ft_ref):
    block, rows = u_ref.shape
    blocks = block // SUB

    def outer(b, carry):
        start = pl.multiple_of(b * SUB, SUB)
        u = u_ref[pl.ds(start, SUB), :]
        m = m_ref[pl.ds(start, SUB), :]
        ft = ft_ref[b, pl.ds(start, SUB), :SUB]
        errors = []
        for s in range(SUB):
            error = jnp.broadcast_to(m[s : s + 1] * u[s : s + 1], (SUB, rows))
            u = u - ft[:, s : s + 1] * error
            errors.append(error)
        u_ref[pl.ds(start, SUB), :] = u
        sub_ids = lax.broadcasted_iota(jnp.int32, (SUB, rows), 0)
        stacked = errors[0]
        for s in range(1, SUB):
            stacked = jnp.where(sub_ids == s, errors[s], stacked)
        e_ref[pl.ds(start, SUB), :] = stacked

        def inner(c, carry):
            place = pl.multiple_of(c * SUB, SUB)
            later = u_ref[pl.ds(place, SUB), :]
            column = ft_ref[b, pl.ds(place, SUB), :SUB]
            for s in range(SUB):
                later = later - column[:, s : s + 1] * errors[s]
            u_ref[pl.ds(place, SUB), :] = later
            return carry

        return lax.fori_loop(b + 1, blocks, inner, carry)

    lax.fori_loop(first, last, outer, 0)


def prune_trailing(w_ref, f_ref, out_ref, u_ref, e_ref, lhs_ref, rhs_ref):
    width = w_ref.shape[1]
    block = u_ref.shape[0]
    errors = e_ref[...].T
    high = errors.astype(jnp.bfloat16)
    low = (errors - high.astype(jnp.float32)).astype(jnp.bfloat16)
    lhs_ref[:, :block] = high
    lhs_ref[:, block : 2 * block] = low
    lhs_ref[:, 2 * block :] = high
    f_high = f_ref[...].astype(jnp.bfloat16)
    f_low = (f_ref[...] - f_high.astype(jnp.float32)).astype(jnp.bfloat16)
    rhs_ref[:block] = f_high
    rhs_ref[block : 2 * block] = f_high
    rhs_ref[2 * block :] = f_low
    out_ref[:, :block] = u_ref[...].T.astype(jnp.bfloat16)
    tile = next(t for t in (3 * LANES, 2 * LANES, LANES) if (width - block) % t == 0)

    def trail(c, carry):
        cols = pl.ds(pl.multiple_of(block + c * tile, LANES), tile)
        change = jnp.dot(lhs_ref[...], rhs_ref[:, cols], preferred_element_type=jnp.float32)
        out_ref[:, cols] = (w_ref[:, cols].astype(jnp.float32) - change).astype(jnp.bfloat16)
        return carry

    lax.fori_loop(0, (width - block) // tile, trail, 0)


def prune_kernel(w_ref, mask_ref, f_ref, out_ref, u_ref, e_ref, m_ref, ft_ref, lhs_ref, rhs_ref):
    prune_setup(w_ref, mask_ref, f_ref, u_ref, m_ref, ft_ref)
    prune_columns(0, u_ref.shape[0] // SUB, u_ref, e_ref, m_ref, ft_ref)
    prune_trailing(w_ref, f_ref, out_ref, u_ref, e_ref, lhs_ref, rhs_ref)


def prune_scratch(rows, width, block):
    return [
        VMEM((block, rows), jnp.float32),
        VMEM((block, rows), jnp.float32),
        VMEM((block, rows), jnp.float32),
        VMEM((block // SUB, block, LANES), jnp.float32),
        VMEM((rows, 3 * block), jnp.bfloat16),
        VMEM((3 * block, width), jnp.bfloat16),
    ]


def prune(weights, keep_mask, inv_factor):
    rows, width = weights.shape
    block = keep_mask.shape[1]
    return pl.pallas_call(
        prune_kernel,
        out_shape=jax.ShapeDtypeStruct((rows, width), jnp.bfloat16),
        in_specs=[pl.BlockSpec(memory_space=VMEM)] * 3,
        out_specs=pl.BlockSpec(memory_space=VMEM),
        scratch_shapes=prune_scratch(rows, width, block),
        cost_estimate=pl.CostEstimate(
            flops=6 * rows * block * width, bytes_accessed=4 * rows * width, transcendentals=0
        ),
        name="prune",
    )(weights, keep_mask, inv_factor)


def remote(src, dst, send_sem, recv_sem, device):
    return pltpu.make_async_remote_copy(
        src_ref=src,
        dst_ref=dst,
        send_sem=send_sem,
        recv_sem=recv_sem,
        device_id=device,
        device_id_type=pl.DeviceIdType.MESH,
    )


def fused_kernel(
    owners, capacity, own_ref, target_ref, w_any, mask_any, f_any, out_ref,
    u_ref, e_ref, m_ref, ft_ref, lhs_ref, rhs_ref,
    w_ref, mask_ref, f_ref, pruned_ref, tokens_ref, packed_ref, back_ref, pick_ref,
    load_sem, line_sem, x_sem, y_sem, core_sem, in_sem, return_sem, back_sem,
):
    width = w_ref.shape[1]
    rows = own_ref.shape[0]
    half_rows = rows // 2
    devices = packed_ref.shape[0]
    hidden_half = w_ref.shape[0] // 2
    line = owners // 4
    x = lax.axis_index("dp")
    expert = lax.axis_index("expert")
    z, y, core = expert // 4, (expert // 2) % 2, expert % 2
    me = x * owners + expert
    other_x, other_y, other_core = 1 - x, 1 - y, 1 - core

    def expert_of(zz, yy, cc):
        return zz * 4 + yy * 2 + cc

    def part(n, first, count):
        return tokens_ref.at[pl.ds(pl.multiple_of(n * rows + first, SUB * 2), count)]

    x_to = (other_x, expert)
    y_to = (x, expert_of(z, other_y, core))
    core_to = (x, expert_of(z, y, other_core))

    def level(r):
        return (z + r) % line

    def block_of(r, xx, yy, cc):
        return xx * owners + expert_of(level(r), yy, cc)

    def to_line(r):
        there = (z + line - r) % line
        return remote(
            own_ref, part(me, 0, rows), line_sem.at[r], in_sem.at[me, 0],
            (x, expert_of(there, y, core)),
        )

    def whole(src, n, sem, to):
        return remote(src, part(n, 0, rows), sem, in_sem.at[n, 0], to)

    def source(r):
        return own_ref if isinstance(r, int) and r == 0 else part(block_of(r, x, y, core), 0, rows)

    def plane_sends(r):
        n = block_of(r, x, y, core)
        return [
            whole(source(r), n, x_sem.at[r, 0], x_to),
            whole(source(r), n, y_sem.at[r, 0], y_to),
            whole(source(r), n, core_sem.at[r, 0], core_to),
        ]

    def diagonal_sends(r):
        n_y = block_of(r, x, other_y, core)
        n_x = block_of(r, other_x, y, core)
        upper, lower = part(n_y, 0, half_rows), part(n_x, half_rows, half_rows)
        return [
            remote(upper, upper, x_sem.at[r, 1], in_sem.at[n_y, 0], x_to),
            remote(lower, lower, y_sem.at[r, 1], in_sem.at[n_x, 1], y_to),
        ]

    def side_sends(r):
        n_y = block_of(r, x, other_y, core)
        n_x = block_of(r, other_x, y, core)
        return [
            whole(part(n_y, 0, rows), n_y, core_sem.at[r, 1], core_to),
            whole(part(n_x, 0, rows), n_x, core_sem.at[r, 2], core_to),
        ]

    def last_sends(r):
        n = block_of(r, other_x, other_y, core)
        return [whole(part(n, 0, rows), n, core_sem.at[r, 3], core_to)]

    def arrive(n):
        whole(part(n, 0, rows), n, core_sem.at[0, 0], core_to).wait_recv()

    def arrive_half(n, h):
        piece = part(n, h * half_rows, half_rows)
        remote(piece, piece, core_sem.at[0, 0], in_sem.at[n, h], core_to).wait_recv()

    def start(copies):
        for copy in copies:
            copy.start()

    def first_stage(r):
        arrive(block_of(r, x, y, core))
        start(plane_sends(r))

    def second_stage(r):
        arrive(block_of(r, x, other_y, core))
        arrive(block_of(r, other_x, y, core))
        start(diagonal_sends(r) + side_sends(r))

    def give_back(n):
        return remote(
            packed_ref.at[n], back_ref.at[me], return_sem.at[n], back_sem.at[me],
            (n // owners, n % owners),
        )

    def apply(r):
        n = block_of(r, other_x, other_y, core)
        arrive_half(n, 0)
        arrive_half(n, 1)
        start(last_sends(r))
        for xx in range(2):
            for yy in range(2):
                arrive(block_of(r, xx, yy, other_core))

        def group(g, carry):
            first = g * owners + level(r) * 4
            span = pl.ds(pl.multiple_of(first * rows, SUB * 2), 4 * rows)
            both = lax.dot_general(
                tokens_ref[span, :width], pruned_ref[...], (((1,), (1,)), ((), ())),
                preferred_element_type=jnp.float32,
            )
            gate, up = both[:, :hidden_half], both[:, hidden_half:]
            hidden = (gate / (1.0 + jnp.exp(-gate)) * up).astype(jnp.bfloat16)
            ranks = tokens_ref[span, width:].astype(jnp.float32)
            lane = lax.broadcasted_iota(jnp.int32, ranks.shape, 1)
            rank = jnp.sum(jnp.where(lane == expert, ranks, 0.0), axis=1, keepdims=True)
            slots = lax.broadcasted_iota(jnp.int32, (4 * rows, capacity), 1).astype(jnp.float32)
            pick = jnp.where(rank == slots, 1.0, 0.0).astype(jnp.bfloat16)
            for j in range(4):
                mine = slice(j * rows, (j + 1) * rows)
                packed_ref[first + j] = lax.dot_general(
                    pick[mine], hidden[mine], (((0,), (0,)), ((), ())),
                    preferred_element_type=jnp.float32,
                ).astype(jnp.bfloat16)
            for j in range(4):
                n = first + j

                @pl.when(n == me)
                def _():
                    back_ref[me] = packed_ref[me]

                @pl.when(n != me)
                def _():
                    give_back(n).start()

            return carry

        lax.fori_loop(0, 2, group, 0)

    loads = [
        pltpu.make_async_copy(w_any, w_ref, load_sem.at[0]),
        pltpu.make_async_copy(mask_any, mask_ref, load_sem.at[1]),
        pltpu.make_async_copy(f_any, f_ref, load_sem.at[2]),
    ]
    start(loads)
    for r in range(1, line):
        to_line(r).start()
    start(plane_sends(0))
    tokens_ref[pl.ds(pl.multiple_of(me * rows, SUB * 2), rows), :] = own_ref[...]
    for load in loads:
        load.wait()
    blocks = u_ref.shape[0] // SUB
    prune_setup(w_ref, mask_ref, f_ref, u_ref, m_ref, ft_ref)
    prune_columns(0, blocks // 2, u_ref, e_ref, m_ref, ft_ref)
    second_stage(0)
    prune_columns(blocks // 2, blocks, u_ref, e_ref, m_ref, ft_ref)
    first_stage(1)
    prune_trailing(w_ref, f_ref, pruned_ref, u_ref, e_ref, lhs_ref, rhs_ref)
    second_stage(1)
    apply(0)

    def middle(r, carry):
        first_stage(r)
        second_stage(r)
        apply(r - 1)
        return carry

    lax.fori_loop(2, line, middle, 0)
    apply(line - 1)
    place = lax.broadcasted_iota(jnp.int32, pick_ref.shape, 1)
    pick_ref[...] = jnp.where(target_ref[...] == place, 1.0, 0.0).astype(jnp.bfloat16)

    def settle(n, carry):
        @pl.when(n != me)
        def _():
            remote(
                packed_ref.at[n], back_ref.at[n], return_sem.at[n], back_sem.at[n], x_to
            ).wait_recv()
            give_back(n).wait_send()

        return carry

    lax.fori_loop(0, devices, settle, 0)
    for h in range(2):
        got = back_ref[pl.ds(h * owners, owners)].reshape(owners * capacity, hidden_half)
        out_ref[:, h * hidden_half : (h + 1) * hidden_half] = jnp.dot(
            pick_ref[...], got, preferred_element_type=jnp.float32
        ).astype(jnp.bfloat16)
    for r in range(line):
        if r:
            to_line(r).wait_send()
        for copy in plane_sends(r) + diagonal_sends(r) + side_sends(r) + last_sends(r):
            copy.wait_send()


def ranks_of(routes, owners):
    token_rows = routes.shape[0]
    ids = jnp.arange(owners, dtype=jnp.int32)
    hot = jnp.any(routes[:, :, None] == ids[None, None, :], axis=1)
    before = jnp.tril(jnp.ones((token_rows, token_rows), jnp.bfloat16), -1)
    rank = jnp.dot(before, hot.astype(jnp.bfloat16), preferred_element_type=jnp.float32)
    return jnp.where(hot, rank, -1.0)


def dense(tokens, routes, weights, keep_mask, inv_factor, capacity):
    owners, groups = lax.axis_size("expert"), lax.axis_size("dp")
    token_rows, width = tokens.shape
    top = routes.shape[1]
    devices = owners * groups
    block = keep_mask.shape[1]
    rows = weights.shape[0]
    half = rows // 2
    line = owners // 4
    rank = ranks_of(routes, owners)
    extra = -owners % LANES
    tagged = jnp.concatenate(
        [tokens, jnp.pad(rank, ((0, 0), (0, extra))).astype(jnp.bfloat16)], axis=1
    )
    ids = jnp.arange(owners, dtype=jnp.int32)
    own_rank = jnp.sum(
        jnp.where(routes[:, :, None] == ids[None, None, :], rank[:, None, :], 0.0), axis=2
    ).astype(jnp.int32)
    target = (routes * capacity + own_rank).reshape(-1, 1)
    dma = pltpu.SemaphoreType.DMA
    out = pl.pallas_call(
        functools.partial(fused_kernel, owners, capacity),
        out_shape=jax.ShapeDtypeStruct((token_rows * top, groups * half), jnp.bfloat16),
        in_specs=[pl.BlockSpec(memory_space=VMEM)] * 2 + [pl.BlockSpec(memory_space=pl.ANY)] * 3,
        out_specs=pl.BlockSpec(memory_space=VMEM),
        scratch_shapes=prune_scratch(rows, width, block)
        + [
            VMEM(weights.shape, weights.dtype),
            VMEM(keep_mask.shape, keep_mask.dtype),
            VMEM(inv_factor.shape, inv_factor.dtype),
            VMEM(weights.shape, jnp.bfloat16),
            VMEM((devices * token_rows, tagged.shape[1]), jnp.bfloat16),
            VMEM((devices, capacity, half), jnp.bfloat16),
            VMEM((devices, capacity, half), jnp.bfloat16),
            VMEM((token_rows * top, owners * capacity), jnp.bfloat16),
            dma((3,)),
            dma((line,)),
            dma((line, 2)),
            dma((line, 2)),
            dma((line, 4)),
            dma((devices, 2)),
            dma((devices,)),
            dma((devices,)),
        ],
        compiler_params=pltpu.CompilerParams(
            has_side_effects=True, vmem_limit_bytes=60 << 20
        ),
        name="fused",
    )(tagged, target, weights, keep_mask, inv_factor)
    return out.reshape(token_rows, top, groups * half)


def routed(tokens, routes, pruned, capacity):
    half = pruned.shape[0] // 2
    gate_all = lax.all_gather(pruned[:half], "dp", axis=0, tiled=True)
    up_all = lax.all_gather(pruned[half:], "dp", axis=0, tiled=True)
    owners = lax.axis_size("expert")
    token_rows, model_width = tokens.shape
    top_count = routes.shape[1]
    slot_expert = routes.reshape(-1)
    one_hot = (slot_expert[:, None] == jnp.arange(owners, dtype=jnp.int32)[None, :]).astype(
        jnp.int32
    )
    slot_rank = jnp.sum(jnp.cumsum(one_hot, axis=0) * one_hot, axis=1) - 1
    target = slot_expert * capacity + slot_rank
    source = jnp.arange(slot_expert.shape[0], dtype=jnp.int32) // top_count
    outbox = (
        jnp.zeros((owners * capacity, model_width), jnp.bfloat16).at[target].set(tokens[source])
    )
    outbox = outbox.reshape(owners, capacity, model_width)
    arrived = lax.all_to_all(outbox, "expert", split_axis=0, concat_axis=0, tiled=True)
    arrived_rows = arrived.reshape(-1, model_width)
    gate_out = lax.dot_general(
        arrived_rows, gate_all, (((1,), (1,)), ((), ())), preferred_element_type=jnp.float32
    )
    up_out = lax.dot_general(
        arrived_rows, up_all, (((1,), (1,)), ((), ())), preferred_element_type=jnp.float32
    )
    hidden_rows = (jax.nn.silu(gate_out) * up_out).astype(jnp.bfloat16)
    hidden_rows = hidden_rows.reshape(arrived.shape[0], arrived.shape[1], -1)
    results = lax.all_to_all(hidden_rows, "expert", split_axis=0, concat_axis=0, tiled=True)
    hidden = results.reshape(owners * capacity, -1)[target]
    return hidden.reshape(token_rows, top_count, -1)


def local(tokens, routes, weights, keep_mask, inv_factor):
    owners, groups = lax.axis_size("expert"), lax.axis_size("dp")
    token_rows, width = tokens.shape
    capacity = token_rows * routes.shape[1] * 4 // (3 * owners)
    weights = weights.reshape(-1, width)
    keep_mask = keep_mask.reshape(-1, keep_mask.shape[-1])
    inv_factor = inv_factor.reshape(-1, width)
    fits = 2 * owners * groups * tokens.size <= GATHER_LIMIT
    if fits and groups == 2 and owners % 4 == 0 and owners >= 8 and token_rows % 32 == 0:
        return dense(tokens, routes, weights, keep_mask, inv_factor, capacity)
    return routed(tokens, routes, prune(weights, keep_mask, inv_factor), capacity)


def solution(mesh):
    return jax.shard_map(
        local,
        mesh=mesh,
        in_specs=(
            P(("dp", "expert"), None),
            P(("dp", "expert"), None),
            P("expert", None, "dp", None),
            P("expert", None, "dp", None),
            P("expert", None, None),
        ),
        out_specs=P(("dp", "expert"), None, None),
        check_vma=False,
    )
```

```python
import functools

import jax
import jax.numpy as jnp
from jax import lax
from jax.experimental import pallas as pl
from jax.experimental.pallas import tpu as pltpu
from jax.sharding import PartitionSpec as P

SUB = 8
LANES = 128
GATHER_LIMIT = 24 << 20
VMEM = pltpu.VMEM


def prune_setup(w_ref, mask_ref, f_ref, u_ref, m_ref, ft_ref):
    block = mask_ref.shape[1]
    u_ref[...] = w_ref[:, :block].astype(jnp.float32).T
    factor = f_ref[:, :block]
    eye = lax.broadcasted_iota(jnp.int32, (block, block), 0) == lax.broadcasted_iota(
        jnp.int32, (block, block), 1
    )
    diagonal = jnp.sum(jnp.where(eye, factor, 0.0), axis=1, keepdims=True)
    m_ref[...] = (1 - mask_ref[...]).astype(jnp.float32).T * (1.0 / diagonal)
    factor_t = factor.T
    for b in range(block // SUB):
        ft_ref[b, :, :SUB] = factor_t[:, b * SUB : (b + 1) * SUB]


def prune_columns(first, last, u_ref, e_ref, m_ref, ft_ref):
    block, rows = u_ref.shape
    blocks = block // SUB

    def outer(b, carry):
        start = pl.multiple_of(b * SUB, SUB)
        u = u_ref[pl.ds(start, SUB), :]
        m = m_ref[pl.ds(start, SUB), :]
        ft = ft_ref[b, pl.ds(start, SUB), :SUB]
        errors = []
        for s in range(SUB):
            error = jnp.broadcast_to(m[s : s + 1] * u[s : s + 1], (SUB, rows))
            u = u - ft[:, s : s + 1] * error
            errors.append(error)
        u_ref[pl.ds(start, SUB), :] = u
        sub_ids = lax.broadcasted_iota(jnp.int32, (SUB, rows), 0)
        stacked = errors[0]
        for s in range(1, SUB):
            stacked = jnp.where(sub_ids == s, errors[s], stacked)
        e_ref[pl.ds(start, SUB), :] = stacked

        def inner(c, carry):
            place = pl.multiple_of(c * SUB, SUB)
            later = u_ref[pl.ds(place, SUB), :]
            column = ft_ref[b, pl.ds(place, SUB), :SUB]
            for s in range(SUB):
                later = later - column[:, s : s + 1] * errors[s]
            u_ref[pl.ds(place, SUB), :] = later
            return carry

        return lax.fori_loop(b + 1, blocks, inner, carry)

    lax.fori_loop(first, last, outer, 0)


def prune_trailing(w_ref, f_ref, out_ref, u_ref, e_ref, lhs_ref, rhs_ref):
    width = w_ref.shape[1]
    block = u_ref.shape[0]
    errors = e_ref[...].T
    high = errors.astype(jnp.bfloat16)
    low = (errors - high.astype(jnp.float32)).astype(jnp.bfloat16)
    lhs_ref[:, :block] = high
    lhs_ref[:, block : 2 * block] = low
    lhs_ref[:, 2 * block :] = high
    f_high = f_ref[...].astype(jnp.bfloat16)
    f_low = (f_ref[...] - f_high.astype(jnp.float32)).astype(jnp.bfloat16)
    rhs_ref[:block] = f_high
    rhs_ref[block : 2 * block] = f_high
    rhs_ref[2 * block :] = f_low
    out_ref[:, :block] = u_ref[...].T.astype(jnp.bfloat16)
    tile = next(t for t in (3 * LANES, 2 * LANES, LANES) if (width - block) % t == 0)

    def trail(c, carry):
        cols = pl.ds(pl.multiple_of(block + c * tile, LANES), tile)
        change = jnp.dot(lhs_ref[...], rhs_ref[:, cols], preferred_element_type=jnp.float32)
        out_ref[:, cols] = (w_ref[:, cols].astype(jnp.float32) - change).astype(jnp.bfloat16)
        return carry

    lax.fori_loop(0, (width - block) // tile, trail, 0)


def prune_kernel(w_ref, mask_ref, f_ref, out_ref, u_ref, e_ref, m_ref, ft_ref, lhs_ref, rhs_ref):
    prune_setup(w_ref, mask_ref, f_ref, u_ref, m_ref, ft_ref)
    prune_columns(0, u_ref.shape[0] // SUB, u_ref, e_ref, m_ref, ft_ref)
    prune_trailing(w_ref, f_ref, out_ref, u_ref, e_ref, lhs_ref, rhs_ref)


def prune_scratch(rows, width, block):
    return [
        VMEM((block, rows), jnp.float32),
        VMEM((block, rows), jnp.float32),
        VMEM((block, rows), jnp.float32),
        VMEM((block // SUB, block, LANES), jnp.float32),
        VMEM((rows, 3 * block), jnp.bfloat16),
        VMEM((3 * block, width), jnp.bfloat16),
    ]


def prune(weights, keep_mask, inv_factor):
    rows, width = weights.shape
    block = keep_mask.shape[1]
    return pl.pallas_call(
        prune_kernel,
        out_shape=jax.ShapeDtypeStruct((rows, width), jnp.bfloat16),
        in_specs=[pl.BlockSpec(memory_space=VMEM)] * 3,
        out_specs=pl.BlockSpec(memory_space=VMEM),
        scratch_shapes=prune_scratch(rows, width, block),
        cost_estimate=pl.CostEstimate(
            flops=6 * rows * block * width, bytes_accessed=4 * rows * width, transcendentals=0
        ),
        name="prune",
    )(weights, keep_mask, inv_factor)


def remote(src, dst, send_sem, recv_sem, device):
    return pltpu.make_async_remote_copy(
        src_ref=src,
        dst_ref=dst,
        send_sem=send_sem,
        recv_sem=recv_sem,
        device_id=device,
        device_id_type=pl.DeviceIdType.MESH,
    )


def fused_kernel(
    owners, capacity, own_ref, own_rank_ref, target_ref, w_any, mask_any, f_any, out_ref,
    u_ref, e_ref, m_ref, ft_ref, lhs_ref, rhs_ref,
    w_ref, mask_ref, f_ref, pruned_ref, tokens_ref, ranks_ref, packed_ref, back_ref,
    pick_ref, rank_sem, rank_in_sem, load_sem, line_sem, x_sem, y_sem, core_sem, in_sem, return_sem, back_sem,
):
    width = w_ref.shape[1]
    rows = own_ref.shape[0]
    half_rows = rows // 2
    devices = packed_ref.shape[0]
    hidden_half = w_ref.shape[0] // 2
    line = owners // 4
    x = lax.axis_index("dp")
    expert = lax.axis_index("expert")
    z, y, core = expert // 4, (expert // 2) % 2, expert % 2
    me = x * owners + expert
    other_x, other_y, other_core = 1 - x, 1 - y, 1 - core

    def expert_of(zz, yy, cc):
        return zz * 4 + yy * 2 + cc

    def part(n, first, count):
        return tokens_ref.at[pl.ds(pl.multiple_of(n * rows + first, SUB * 2), count)]

    x_to = (other_x, expert)
    y_to = (x, expert_of(z, other_y, core))
    core_to = (x, expert_of(z, y, other_core))

    def level(r):
        return (z + r) % line

    def block_of(r, xx, yy, cc):
        return xx * owners + expert_of(level(r), yy, cc)

    def to_line(r):
        there = (z + line - r) % line
        return remote(
            own_ref, part(me, 0, rows), line_sem.at[r], in_sem.at[me, 0],
            (x, expert_of(there, y, core)),
        )

    def whole(src, n, sem, to):
        return remote(src, part(n, 0, rows), sem, in_sem.at[n, 0], to)

    def source(r):
        return own_ref if isinstance(r, int) and r == 0 else part(block_of(r, x, y, core), 0, rows)

    def half_send(src, n, h, sem, to):
        piece = part(n, h * half_rows, half_rows)
        if src is own_ref:
            return remote(src.at[pl.ds(h * half_rows, half_rows)], piece, sem, in_sem.at[n, h], to)
        return remote(piece, piece, sem, in_sem.at[n, h], to)

    def plane_sends(r):
        n = block_of(r, x, y, core)
        return [
            half_send(source(r), n, 1, x_sem.at[r, 0], x_to),
            half_send(source(r), n, 0, y_sem.at[r, 0], y_to),
            half_send(source(r), n, 0, x_sem.at[r, 2], x_to),
            half_send(source(r), n, 1, y_sem.at[r, 2], y_to),
            whole(source(r), n, core_sem.at[r, 0], core_to),
        ]

    def diagonal_sends(r):
        n_y = block_of(r, x, other_y, core)
        n_x = block_of(r, other_x, y, core)
        upper, lower = part(n_y, 0, half_rows), part(n_x, half_rows, half_rows)
        return [
            remote(upper, upper, x_sem.at[r, 1], in_sem.at[n_y, 0], x_to),
            remote(lower, lower, y_sem.at[r, 1], in_sem.at[n_x, 1], y_to),
        ]

    def side_sends(r):
        n_y = block_of(r, x, other_y, core)
        n_x = block_of(r, other_x, y, core)
        return [
            whole(part(n_y, 0, rows), n_y, core_sem.at[r, 1], core_to),
            whole(part(n_x, 0, rows), n_x, core_sem.at[r, 2], core_to),
        ]

    def last_sends(r):
        n = block_of(r, other_x, other_y, core)
        return [whole(part(n, 0, rows), n, core_sem.at[r, 3], core_to)]

    def arrive(n):
        whole(part(n, 0, rows), n, core_sem.at[0, 0], core_to).wait_recv()

    def arrive_half(n, h):
        piece = part(n, h * half_rows, half_rows)
        remote(piece, piece, core_sem.at[0, 0], in_sem.at[n, h], core_to).wait_recv()

    def start(copies):
        for copy in copies:
            copy.start()

    def first_stage(r):
        arrive(block_of(r, x, y, core))
        start(plane_sends(r))

    def second_stage(r):
        upward, across = diagonal_sends(r)
        arrive_half(block_of(r, x, other_y, core), 0)
        upward.start()
        arrive_half(block_of(r, other_x, y, core), 1)
        across.start()

    def third_stage(r):
        arrive_half(block_of(r, x, other_y, core), 1)
        arrive_half(block_of(r, other_x, y, core), 0)
        start(side_sends(r))

    def rank_send(n):
        return remote(
            own_rank_ref.at[n % owners], ranks_ref.at[me], rank_sem.at[n], rank_in_sem.at[me],
            (n // owners, n % owners),
        )

    def give_back(n):
        return remote(
            packed_ref.at[n], back_ref.at[me], return_sem.at[n], back_sem.at[me],
            (n // owners, n % owners),
        )

    def apply(r):
        n = block_of(r, other_x, other_y, core)
        arrive_half(n, 0)
        arrive_half(n, 1)
        start(last_sends(r))
        for xx in range(2):
            for yy in range(2):
                arrive(block_of(r, xx, yy, other_core))

        def group(g, carry):
            first = g * owners + level(r) * 4
            span = pl.ds(pl.multiple_of(first * rows, SUB * 2), 4 * rows)
            both = lax.dot_general(
                tokens_ref[span, :], pruned_ref[...], (((1,), (1,)), ((), ())),
                preferred_element_type=jnp.float32,
            )
            gate, up = both[:, :hidden_half], both[:, hidden_half:]
            hidden = (gate / (1.0 + jnp.exp(-gate)) * up).astype(jnp.bfloat16)
            slots = lax.broadcasted_iota(jnp.int32, (capacity, rows), 0).astype(jnp.float32)
            for j in range(4):
                rank = ranks_ref[first + j][:, :rows]
                pick = jnp.where(rank == slots, 1.0, 0.0).astype(jnp.bfloat16)
                packed_ref[first + j] = jnp.dot(
                    pick, hidden[j * rows : (j + 1) * rows], preferred_element_type=jnp.float32
                ).astype(jnp.bfloat16)
            for j in range(4):
                n = first + j

                @pl.when(n == me)
                def _():
                    back_ref[me] = packed_ref[me]

                @pl.when(n != me)
                def _():
                    give_back(n).start()

            return carry

        lax.fori_loop(0, 2, group, 0)

    loads = [
        pltpu.make_async_copy(w_any, w_ref, load_sem.at[0]),
        pltpu.make_async_copy(mask_any, mask_ref, load_sem.at[1]),
        pltpu.make_async_copy(f_any, f_ref, load_sem.at[2]),
    ]
    start(loads)
    for r in range(1, line):
        to_line(r).start()
    start(plane_sends(0))

    def share_rank(k, carry):
        rank_send((me + k) % devices).start()
        return carry

    lax.fori_loop(1, devices, share_rank, 0)
    ranks_ref[me] = own_rank_ref[expert]
    tokens_ref[pl.ds(pl.multiple_of(me * rows, SUB * 2), rows), :] = own_ref[...]
    for load in loads:
        load.wait()
    blocks = u_ref.shape[0] // SUB
    prune_setup(w_ref, mask_ref, f_ref, u_ref, m_ref, ft_ref)
    prune_columns(0, blocks // 2, u_ref, e_ref, m_ref, ft_ref)
    second_stage(0)
    prune_columns(blocks // 2, blocks, u_ref, e_ref, m_ref, ft_ref)
    third_stage(0)
    first_stage(1)
    prune_trailing(w_ref, f_ref, pruned_ref, u_ref, e_ref, lhs_ref, rhs_ref)
    second_stage(1)

    def know_rank(n, carry):
        @pl.when(n != me)
        def _():
            remote(
                own_rank_ref.at[0], ranks_ref.at[n], rank_sem.at[n], rank_in_sem.at[n], x_to
            ).wait_recv()
            rank_send(n).wait_send()

        return carry

    lax.fori_loop(0, devices, know_rank, 0)
    apply(0)
    third_stage(1)

    def middle(r, carry):
        first_stage(r)
        second_stage(r)
        apply(r - 1)
        third_stage(r)
        return carry

    lax.fori_loop(2, line, middle, 0)
    apply(line - 1)
    place = lax.broadcasted_iota(jnp.int32, pick_ref.shape, 1)
    pick_ref[...] = jnp.where(target_ref[...] == place, 1.0, 0.0).astype(jnp.bfloat16)

    def settle(n, carry):
        @pl.when(n != me)
        def _():
            remote(
                packed_ref.at[n], back_ref.at[n], return_sem.at[n], back_sem.at[n], x_to
            ).wait_recv()
            give_back(n).wait_send()

        return carry

    lax.fori_loop(0, devices, settle, 0)
    for h in range(2):
        got = back_ref[pl.ds(h * owners, owners)].reshape(owners * capacity, hidden_half)
        out_ref[:, h * hidden_half : (h + 1) * hidden_half] = jnp.dot(
            pick_ref[...], got, preferred_element_type=jnp.float32
        ).astype(jnp.bfloat16)
    for r in range(line):
        if r:
            to_line(r).wait_send()
        for copy in plane_sends(r) + diagonal_sends(r) + side_sends(r) + last_sends(r):
            copy.wait_send()


def ranks_of(routes, owners):
    token_rows = routes.shape[0]
    ids = jnp.arange(owners, dtype=jnp.int32)
    hot = jnp.any(routes[:, :, None] == ids[None, None, :], axis=1)
    before = jnp.tril(jnp.ones((token_rows, token_rows), jnp.bfloat16), -1)
    rank = jnp.dot(before, hot.astype(jnp.bfloat16), preferred_element_type=jnp.float32)
    return jnp.where(hot, rank, -1.0)


def dense(tokens, routes, weights, keep_mask, inv_factor, capacity):
    owners, groups = lax.axis_size("expert"), lax.axis_size("dp")
    token_rows, width = tokens.shape
    top = routes.shape[1]
    devices = owners * groups
    block = keep_mask.shape[1]
    rows = weights.shape[0]
    half = rows // 2
    line = owners // 4
    rank = ranks_of(routes, owners)
    rank_rows = jnp.pad(rank.T, ((0, 0), (0, -token_rows % LANES)))[:, None, :]
    ids = jnp.arange(owners, dtype=jnp.int32)
    own_rank = jnp.sum(
        jnp.where(routes[:, :, None] == ids[None, None, :], rank[:, None, :], 0.0), axis=2
    ).astype(jnp.int32)
    target = (routes * capacity + own_rank).reshape(-1, 1)
    dma = pltpu.SemaphoreType.DMA
    out = pl.pallas_call(
        functools.partial(fused_kernel, owners, capacity),
        out_shape=jax.ShapeDtypeStruct((token_rows * top, groups * half), jnp.bfloat16),
        in_specs=[pl.BlockSpec(memory_space=VMEM)] * 3 + [pl.BlockSpec(memory_space=pl.ANY)] * 3,
        out_specs=pl.BlockSpec(memory_space=VMEM),
        scratch_shapes=prune_scratch(rows, width, block)
        + [
            VMEM(weights.shape, weights.dtype),
            VMEM(keep_mask.shape, keep_mask.dtype),
            VMEM(inv_factor.shape, inv_factor.dtype),
            VMEM(weights.shape, jnp.bfloat16),
            VMEM((devices * token_rows, width), jnp.bfloat16),
            VMEM((devices,) + rank_rows.shape[1:], jnp.float32),
            VMEM((devices, capacity, half), jnp.bfloat16),
            VMEM((devices, capacity, half), jnp.bfloat16),
            VMEM((token_rows * top, owners * capacity), jnp.bfloat16),
            dma((devices,)),
            dma((devices,)),
            dma((3,)),
            dma((line,)),
            dma((line, 3)),
            dma((line, 3)),
            dma((line, 4)),
            dma((devices, 2)),
            dma((devices,)),
            dma((devices,)),
        ],
        compiler_params=pltpu.CompilerParams(
            has_side_effects=True, vmem_limit_bytes=60 << 20
        ),
        name="fused",
    )(tokens, rank_rows, target, weights, keep_mask, inv_factor)
    return out.reshape(token_rows, top, groups * half)


def routed(tokens, routes, pruned, capacity):
    half = pruned.shape[0] // 2
    gate_all = lax.all_gather(pruned[:half], "dp", axis=0, tiled=True)
    up_all = lax.all_gather(pruned[half:], "dp", axis=0, tiled=True)
    owners = lax.axis_size("expert")
    token_rows, model_width = tokens.shape
    top_count = routes.shape[1]
    slot_expert = routes.reshape(-1)
    one_hot = (slot_expert[:, None] == jnp.arange(owners, dtype=jnp.int32)[None, :]).astype(
        jnp.int32
    )
    slot_rank = jnp.sum(jnp.cumsum(one_hot, axis=0) * one_hot, axis=1) - 1
    target = slot_expert * capacity + slot_rank
    source = jnp.arange(slot_expert.shape[0], dtype=jnp.int32) // top_count
    outbox = (
        jnp.zeros((owners * capacity, model_width), jnp.bfloat16).at[target].set(tokens[source])
    )
    outbox = outbox.reshape(owners, capacity, model_width)
    arrived = lax.all_to_all(outbox, "expert", split_axis=0, concat_axis=0, tiled=True)
    arrived_rows = arrived.reshape(-1, model_width)
    gate_out = lax.dot_general(
        arrived_rows, gate_all, (((1,), (1,)), ((), ())), preferred_element_type=jnp.float32
    )
    up_out = lax.dot_general(
        arrived_rows, up_all, (((1,), (1,)), ((), ())), preferred_element_type=jnp.float32
    )
    hidden_rows = (jax.nn.silu(gate_out) * up_out).astype(jnp.bfloat16)
    hidden_rows = hidden_rows.reshape(arrived.shape[0], arrived.shape[1], -1)
    results = lax.all_to_all(hidden_rows, "expert", split_axis=0, concat_axis=0, tiled=True)
    hidden = results.reshape(owners * capacity, -1)[target]
    return hidden.reshape(token_rows, top_count, -1)


def local(tokens, routes, weights, keep_mask, inv_factor):
    owners, groups = lax.axis_size("expert"), lax.axis_size("dp")
    token_rows, width = tokens.shape
    capacity = token_rows * routes.shape[1] * 4 // (3 * owners)
    weights = weights.reshape(-1, width)
    keep_mask = keep_mask.reshape(-1, keep_mask.shape[-1])
    inv_factor = inv_factor.reshape(-1, width)
    fits = 2 * owners * groups * tokens.size <= GATHER_LIMIT
    if fits and groups == 2 and owners % 4 == 0 and owners >= 8 and token_rows % 32 == 0:
        return dense(tokens, routes, weights, keep_mask, inv_factor, capacity)
    return routed(tokens, routes, prune(weights, keep_mask, inv_factor), capacity)


def solution(mesh):
    return jax.shard_map(
        local,
        mesh=mesh,
        in_specs=(
            P(("dp", "expert"), None),
            P(("dp", "expert"), None),
            P("expert", None, "dp", None),
            P("expert", None, "dp", None),
            P("expert", None, None),
        ),
        out_specs=P(("dp", "expert"), None, None),
        check_vma=False,
    )
```
